32 devices in a mesh: dp: 8 (over z, core), height: 4 (over y, x).
Axes of the slice: x: 2, y: 2, z: 4, core: 2. Of those that a mesh axis runs over, the one named last changes fastest.
Arguments:
- latents: bfloat16 [8, 16, 128, 640], P('dp', 'height'), parts along dimension 0, may hold values from -20 to 20
- latent_tangent: bfloat16 [8, 16, 128, 640], P('dp', 'height'), parts along dimension 0, may hold values from -20 to 20
- gain_first: float32 [640], replicated, may hold values from 0.5 to 2
- weight_first: bfloat16 [9, 640, 640], P(None, None, 'height'), may hold values from -0.078125 to 0.078125
- gain_second: float32 [640], replicated, may hold values from 0.5 to 2
- weight_second: bfloat16 [9, 640, 640], P(None, None, 'height'), may hold values from -0.078125 to 0.078125
Outputs:
- block_output: bfloat16 [8, 16, 128, 640], P('dp', 'height'), parts along dimension 0
- output_tangent: bfloat16 [8, 16, 128, 640], P('dp', 'height'), parts along dimension 0
The draws below stay inside these ranges and needn't reach their ends.
There are 8 independent parts, one for each index of `dp`. The reference program is written for one: setup_inputs(seed, part) draws one part's arguments, and reference() takes and returns one part's arrays. A program takes and returns all parts, laid end to end along the dimension named above; an argument that names none is the same for every part. Nothing has to cross between parts.
All inputs are finite; a program needn't handle non-finite values.
Results may differ from the reference program's by a relative error of at most 0.006.
Values may be sent and summed in bfloat16 or wider, within the bound.
A program may use at most 128 MiB of HBM per device.

```python
import math
import jax
import jax.numpy as jnp
from jax import lax

C = 640
GROUPS = 32
WIDTH = 128
H = 16


def rising_field(key, salt):
    folded = jax.random.fold_in(key, salt)
    first_key = jax.random.fold_in(folded, 0)
    row_frac = jnp.arange(H, dtype=jnp.float32) / max(H - 1, 1)
    row_scale = (3.0 ** row_frac)[:, None, None]
    base_values = jnp.clip(jax.random.normal(first_key, (H, WIDTH, C), jnp.float32), -6.0, 6.0)
    field = base_values * row_scale
    return jnp.clip(field, -20.0, 20.0)[None]


def draw_latents(key, part):
    return rising_field(key, 11).astype(jnp.bfloat16)


def draw_latent_tangent(key, part):
    return rising_field(key, 23).astype(jnp.bfloat16)


def block_levels(key, extent, cuts, smallest, top_value):
    def one(dim, shards_of):
        steps = jax.random.uniform(jax.random.fold_in(jax.random.fold_in(key, 6), dim), (shards_of,), jnp.float32, smallest / len(cuts), top_value / len(cuts))
        return jnp.repeat(jnp.exp(steps), extent[dim] // shards_of).reshape((-1,) + (1,) * (len(extent) - dim - 1))

    level = one(*cuts[0])
    for cut in cuts[1:]:
        level = level * one(*cut)
    return level


def noise(key, extent, spread, reach, cuts=(), kind=jnp.bfloat16):
    gain = block_levels(key, extent, cuts, -0.22, 0.18) if cuts else 1.0
    array = jax.random.normal(key, extent, jnp.float32) * spread * gain
    return jnp.minimum(jnp.maximum(array, -reach), reach).astype(kind)


def setup_inputs(seed: int = 0, part: int = 0) -> dict:
    key_list = jax.random.split(jax.random.key(seed), 7)
    part_keys = jax.random.split(jax.random.fold_in(key_list[6], part), 7)
    latents = draw_latents(jax.random.fold_in(jax.random.fold_in(key_list[6], part), 71), part)
    latent_tangent = draw_latent_tangent(jax.random.fold_in(jax.random.fold_in(key_list[6], part), 71), part)
    gain_first = jnp.clip(jnp.exp(jax.random.uniform(key_list[2], (C,), jnp.float32, math.log(0.5), math.log(2.0))), 0.5, 2.0)
    weight_first = noise(key_list[3], (9, C, C), (9 * C) ** -0.5, 0.078125, ((2, 4),))
    gain_second = jnp.clip(jnp.exp(jax.random.uniform(key_list[4], (C,), jnp.float32, math.log(0.5), math.log(2.0))), 0.5, 2.0)
    weight_second = noise(key_list[5], (9, C, C), (9 * C) ** -0.5, 0.078125, ((2, 4),))
    return {"latents": latents, "latent_tangent": latent_tangent, "gain_first": gain_first, "weight_first": weight_first, "gain_second": gain_second, "weight_second": weight_second}


epsilon = 1e-05

def normalize(primal, tangent, gain_vector):
    row_count, col_count, chans = primal.shape
    size = chans // GROUPS
    grouped = primal.reshape(row_count * col_count, GROUPS, size)
    tgrouped = tangent.reshape(row_count * col_count, GROUPS, size)
    group_mean = lax.optimization_barrier(jnp.mean(grouped, axis=(0, 2)))
    tangent_mean = lax.optimization_barrier(jnp.mean(tgrouped, axis=(0, 2)))
    centered = grouped - group_mean[None, :, None]
    tangent_centered = tgrouped - tangent_mean[None, :, None]
    variance = lax.optimization_barrier(jnp.mean(centered * centered, axis=(0, 2)))
    dvariance = 2.0 * lax.optimization_barrier(jnp.mean(centered * tangent_centered, axis=(0, 2)))
    inverse = lax.rsqrt(variance + epsilon)[None, :, None]
    normed = centered * inverse
    dnormed = tangent_centered * inverse - centered * (0.5 * dvariance[None, :, None] * inverse ** 3)
    scaled = normed.reshape(row_count, col_count, chans) * gain_vector
    dscaled = dnormed.reshape(row_count, col_count, chans) * gain_vector
    sigmoid_value = jax.nn.sigmoid(scaled)
    hidden = scaled * sigmoid_value
    dhidden = dscaled * sigmoid_value * (1.0 + scaled * (1.0 - sigmoid_value))
    return (hidden.astype(jnp.bfloat16), dhidden.astype(jnp.bfloat16))

def convolve(hidden, weight):
    row_count, col_count, chans = hidden.shape
    padded = jnp.pad(hidden, ((1, 1), (1, 1), (0, 0)))
    accumulated = jnp.zeros((row_count * col_count, weight.shape[2]), jnp.float32)
    for tap_index in range(9):
        offset_row = tap_index // 3
        offset_col = tap_index % 3
        window = padded[offset_row:offset_row + row_count, offset_col:offset_col + col_count, :].reshape(-1, chans)
        accumulated = accumulated + jnp.dot(window, weight[tap_index], preferred_element_type=jnp.float32)
    return accumulated.reshape(row_count, col_count, -1)

def reference(latents, latent_tangent, gain_first, weight_first, gain_second, weight_second):
    primal = latents[0].astype(jnp.float32)
    tangent = latent_tangent[0].astype(jnp.float32)
    hidden, dhidden = normalize(primal, tangent, gain_first)
    middle = convolve(hidden, weight_first).astype(jnp.bfloat16)
    dmiddle = convolve(dhidden, weight_first).astype(jnp.bfloat16)
    second, dsecond = normalize(middle.astype(jnp.float32), dmiddle.astype(jnp.float32), gain_second)
    result = (primal + convolve(second, weight_second)).astype(jnp.bfloat16)
    dresult = (tangent + convolve(dsecond, weight_second)).astype(jnp.bfloat16)
    return (result[None], dresult[None])
```

```python
import functools

import jax
import jax.numpy as jnp
import numpy as np
from jax import lax
from jax.experimental import pallas as pl
from jax.experimental.pallas import tpu as pltpu
from jax.sharding import PartitionSpec as P

GROUPS = 32
TAPS = 9
AHEAD = 6
FAR = 2
CROSS = 6
DOUBLE = 15


epsilon = 1e-05
F32 = jnp.float32
BF16 = jnp.bfloat16


def fused_kernel(
    n, lat, tan, gain_a, gain_b, weight_a, weight_b, same_group,
    out, dout,
    field, mid, shifted, acc, full, stat, peer_stat,
    load_sem, halo_send, halo_recv, stat_send, stat_recv,
    own_send, near_recv, relay_send, far_recv, pair_send, pair_recv,
    plane_send, plane_recv,
):
    rows, width, chans = lat.shape[1], lat.shape[2], lat.shape[3]
    quarter = chans // n
    half = quarter // 2
    steps = 2 * TAPS
    local = rows * width
    pair = 2 * width
    d = lax.axis_index("dp")
    h = lax.axis_index("height")
    core = lax.rem(d, 2)
    xor1 = h + 1 - 2 * lax.rem(h, 2)
    xor2 = lax.rem(h + 2, n)
    xor3 = xor1 + 2 - 4 * (xor1 // 2)
    other = d + 1 - 2 * core
    peers = (xor1, xor2, xor3)
    plane = lax.rem(d // 2, 2)
    across = d + 2 - 4 * plane

    def start_remote(src, dst, send, recv, dd, hh):
        return pltpu.make_async_remote_copy(
            src_ref=src, dst_ref=dst, send_sem=send, recv_sem=recv,
            device_id={"dp": dd, "height": hh},
            device_id_type=pl.DeviceIdType.MESH,
        )

    barrier = pltpu.get_barrier_semaphore()
    for hh in peers:
        pl.semaphore_signal(barrier, inc=1, device_id={"dp": d, "height": hh}, device_id_type=pl.DeviceIdType.MESH)
    pl.semaphore_signal(barrier, inc=1, device_id={"dp": other, "height": h}, device_id_type=pl.DeviceIdType.MESH)

    pl.semaphore_signal(barrier, inc=1, device_id={"dp": across, "height": h}, device_id_type=pl.DeviceIdType.MESH)

    loads = [
        pltpu.make_async_copy(lat.at[0], field.at[0, pl.ds(1, rows)], load_sem.at[0]),
        pltpu.make_async_copy(tan.at[0], field.at[1, pl.ds(1, rows)], load_sem.at[1]),
    ] + [
        pltpu.make_async_copy(
            w.at[pl.ds(3 * src, 3)],
            full.at[pl.ds(TAPS * i + 3 * dst, 3), pl.ds(pl.multiple_of(h * quarter, 16), quarter)],
            load_sem.at[2 + 3 * i + dst])
        for i, w in enumerate((weight_a, weight_b)) for dst, src in enumerate((1, 0, 2))
    ]
    for c in loads:
        c.start()
    def rows_of(hh, cc):
        return pl.ds(pl.multiple_of(hh * quarter + cc * half, 16), half)

    def shared(s):
        return jnp.logical_and(lax.rem(s, TAPS) != TAPS - 1, s < DOUBLE)

    def fetches(s):
        return jnp.logical_or(lax.rem(lax.rem(s, TAPS), 2) == plane, jnp.logical_not(shared(s)))

    def tap_of(v):
        part = lax.rem(v, TAPS)
        row = part // 3
        return 1 - row + 3 * (row // 2), lax.rem(part, 3)

    def own_copy(s, k, w=None):
        if w is None:
            src = full.at[s, rows_of(h, core)]
        else:
            p, q = tap_of(s)
            src = w.at[3 * p + q, pl.ds(pl.multiple_of(core * half, 16), half)]
        return start_remote(
            src, full.at[s, rows_of(h, core)],
            own_send.at[s, k], near_recv.at[s, k], d, peers[k])

    def relay_copy(s):
        along = jnp.logical_and(lax.rem(lax.rem(s, TAPS) // 2, 2) == 1, jnp.logical_or(h == 0, h == n - 1))
        source = jnp.where(along, xor2, xor1)
        target = jnp.where(along, xor1, xor2)
        block = full.at[s, rows_of(source, core)]
        return start_remote(block, block, relay_send.at[s], far_recv.at[s], d, target)

    def pair_copy(s, k):
        block = full.at[s, rows_of(peers[k], core)]
        return start_remote(block, block, pair_send.at[s, k], pair_recv.at[s, k], other, h)

    def plane_copy(s, k):
        block = full.at[s, rows_of(peers[k], core)]
        return start_remote(block, block, plane_send.at[s, k], plane_recv.at[s, k], across, h)

    def send_own(s):
        @pl.when(jnp.logical_and(fetches(s), s < TAPS))
        def _():
            for k in range(2):
                own_copy(s, k, weight_a).start()

        @pl.when(jnp.logical_and(fetches(s), s >= TAPS))
        def _():
            for k in range(2):
                own_copy(s, k, weight_b).start()

    def pass_on(s, k):
        pair_copy(s, k).start()

        @pl.when(shared(s))
        def _():
            plane_copy(s, k).start()

    def comm(s):
        @pl.when(s + AHEAD < steps)
        def _():
            send_own(s + AHEAD)

        @pl.when(jnp.logical_and(s < steps, fetches(s)))
        def _():
            for k in range(2):
                own_copy(s, k).wait_recv()
            relay_copy(s).start()
            for k in range(2):
                pass_on(s, k)

        f = s - FAR

        @pl.when(jnp.logical_and(jnp.logical_and(f >= 0, f < steps), fetches(f)))
        def _():
            relay_copy(f).wait_recv()
            pass_on(f, 2)

        z = s - CROSS

        @pl.when(jnp.logical_and(jnp.logical_and(z >= 0, z < steps), jnp.logical_not(fetches(z))))
        def _():
            for k in range(3):
                plane_copy(z, k).wait_recv()
                pair_copy(z, k).start()

    def halo_copies(buf, k):
        top = [start_remote(buf.at[f, 1], buf.at[f, rows + 1], halo_send.at[k, 0, f], halo_recv.at[k, 0, f], d, lax.rem(h + n - 1, n)) for f in range(2)]
        low = [start_remote(buf.at[f, rows], buf.at[f, 0], halo_send.at[k, 1, f], halo_recv.at[k, 1, f], d, lax.rem(h + 1, n)) for f in range(2)]
        return top, low

    def halo_start(buf, k, sources=None, fields=(0, 1)):
        def edge_row(f, r):
            return buf.at[f, 1 + r] if sources is None else sources[f].at[0, r]

        @pl.when(h > 0)
        def _():
            for f in fields:
                start_remote(edge_row(f, 0), buf.at[f, rows + 1], halo_send.at[k, 0, f], halo_recv.at[k, 0, f], d, lax.rem(h + n - 1, n)).start()

        @pl.when(h < n - 1)
        def _():
            for f in fields:
                start_remote(edge_row(f, rows - 1), buf.at[f, 0], halo_send.at[k, 1, f], halo_recv.at[k, 1, f], d, lax.rem(h + 1, n)).start()

    def halo_wait(buf, k):
        top, low = halo_copies(buf, k)

        @pl.when(h > 0)
        def _():
            for c in top:
                c.wait_send()
            for c in low:
                c.wait_recv()

        @pl.when(h < n - 1)
        def _():
            for c in low:
                c.wait_send()
            for c in top:
                c.wait_recv()

    def local_stats(buf, k):
        zero = jnp.zeros((1, chans), F32)

        def sums(r, carry):
            return (
                carry[0] + jnp.sum(buf[0, r].astype(F32), axis=0, keepdims=True),
                carry[1] + jnp.sum(buf[1, r].astype(F32), axis=0, keepdims=True),
            )

        total, dtotal = lax.fori_loop(1, rows + 1, sums, (zero, zero))
        mean = total / local
        dmean = dtotal / local

        def moments(r, carry):
            v = buf[0, r].astype(F32) - mean
            dv = buf[1, r].astype(F32) - dmean
            return (
                carry[0] + jnp.sum(v * v, axis=0, keepdims=True),
                carry[1] + jnp.sum(v * dv, axis=0, keepdims=True),
            )

        second, dsecond = lax.fori_loop(1, rows + 1, moments, (zero, zero))
        stat[k, 0:1] = mean
        stat[k, 1:2] = dmean
        stat[k, 2:3] = second
        stat[k, 3:4] = dsecond
        stat[k, 4:8] = jnp.zeros((4, chans), F32)

    def stat_copy(k, j):
        return start_remote(stat.at[k], peer_stat.at[k, j], stat_send.at[k, j], stat_recv.at[k, j], d, peers[j])

    def group_sum(x):
        high = x.astype(BF16)
        rest = x - high.astype(F32)
        middle = rest.astype(BF16)
        low = (rest - middle.astype(F32)).astype(BF16)
        dot = lambda part: jnp.dot(part, same_group[...], preferred_element_type=F32)
        return dot(high) + dot(middle) + dot(low)

    def coefficients(k, gain):
        gain_row = gain[...].reshape(1, chans)
        for j in range(n - 1):
            stat_copy(k, j).wait_recv()
        size = chans // GROUPS
        blocks = [stat[k]] + [peer_stat[k, j] for j in range(n - 1)]
        both = blocks[0]
        for b in blocks[1:]:
            both = both + b
        means = group_sum(both) / (n * size)
        mean, dmean = means[0:1], means[1:2]
        var = jnp.zeros((1, chans), F32)
        dvar = jnp.zeros((1, chans), F32)
        for b in blocks:
            off = b[0:1] - mean
            doff = b[1:2] - dmean
            var = var + (b[2:3] + local * (off * off))
            dvar = dvar + (b[3:4] + local * (off * doff))
        row = lax.broadcasted_iota(jnp.int32, (8, chans), 0)
        packed = jnp.where(row == 0, var, jnp.where(row == 1, dvar, 0.0))
        moments = group_sum(packed) / (n * size * local)
        inverse = lax.rsqrt(moments[0:1] + epsilon)
        scale = gain_row * inverse
        slope = gain_row * (moments[1:2] * inverse * inverse * inverse)
        return mean, dmean, scale, slope

    column = lax.broadcasted_iota(jnp.int32, (width, 1), 0)

    def activate(buf, r, coef, keep):
        mean, dmean, scale, slope = coef
        v = buf[0, r].astype(F32) - mean
        dv = buf[1, r].astype(F32) - dmean
        a = v * scale
        da = dv * scale - v * slope
        s = jax.nn.sigmoid(a)
        hid = a * s
        dhid = da * (s * (1.0 + a * (1.0 - s)))
        if keep is not None:
            hid = jnp.where(keep, hid, 0.0)
            dhid = jnp.where(keep, dhid, 0.0)
        for f, x in ((0, hid), (1, dhid)):
            at = pl.ds(pl.multiple_of(r * pair + f * width, 128), width)
            shifted[1, at] = x.astype(BF16)
            shifted[0, at] = jnp.where(column == 0, 0.0, pltpu.roll(x, 1, 0)).astype(BF16)
            shifted[2, at] = jnp.where(column == width - 1, 0.0, pltpu.roll(x, width - 1, 0)).astype(BF16)

    def activate_rows(buf, coef):
        def one(r, carry):
            activate(buf, r, coef, None)
            return carry
        lax.fori_loop(1, rows + 1, one, 0)

    def activate_halo(buf, coef):
        def one(e, carry):
            r = e * (rows + 1)
            edge = jnp.where(e == 0, 0, n - 1)
            activate(buf, r, coef, h != edge)
            return carry
        lax.fori_loop(0, 2, one, 0)

    def arrive(v):
        for k in range(3):
            pair_copy(v, k).wait_recv()

    def accumulate(v, src, dst, count):
        q = tap_of(v)[1]
        at = pl.ds(pl.multiple_of(dst * pair, 128), count * pair)
        acc[at] += lax.dot_general(
            shifted[q, pl.ds(pl.multiple_of(src * pair, 128), count * pair)], full[v],
            (((1,), (1,)), ((), ())), preferred_element_type=F32)

    def loop(low, high, body):
        def one(v, carry):
            body(v)
            return carry
        lax.fori_loop(low, high, one, 0)

    def center(v):
        comm(v + CROSS + 1)
        arrive(v)
        accumulate(v, 1, 0, rows)

    def inner(v):
        comm(v + CROSS + 1)
        arrive(v)
        p = tap_of(v)[0]
        accumulate(v, 1 + p // 2, 1 - p // 2, rows - 1)

    def edge(v):
        p = tap_of(v)[0]
        accumulate(v, (p // 2) * (rows + 1), (p // 2) * (rows - 1), 1)

    loads[0].wait()
    loads[1].wait()
    local_stats(field, 0)
    pl.semaphore_wait(barrier, n + 1)
    for j in range(n - 1):
        stat_copy(0, j).start()
    for s in range(4):
        send_own(s)
    halo_start(field, 0, (lat, tan), (0,))
    for s in range(4, AHEAD):
        send_own(s)
    comm(0)
    comm(1)
    halo_start(field, 0, (lat, tan), (1,))
    acc[...] = jnp.zeros_like(acc)
    coef = coefficients(0, gain_a)
    comm(2)
    activate_rows(field, coef)
    for c in loads[2:5]:
        c.wait()
    for s in range(3, CROSS + 1):
        comm(s)
    loop(0, 3, center)
    loop(3, TAPS, inner)
    halo_wait(field, 0)
    activate_halo(field, coef)
    loop(3, TAPS, edge)

    for c in loads[5:]:
        c.wait()
    for f in range(2):
        for r in range(rows):
            at = r * pair + f * width
            mid[f, r + 1] = acc[at:at + width].astype(BF16)
    local_stats(mid, 1)
    for j in range(n - 1):
        stat_copy(1, j).start()
    halo_start(mid, 1)
    acc[...] = jnp.zeros_like(acc)
    coef = coefficients(1, gain_b)
    activate_rows(mid, coef)
    loop(TAPS, TAPS + 3, center)
    loop(TAPS + 3, steps - 1, inner)
    halo_wait(mid, 1)
    activate_halo(mid, coef)
    loop(TAPS + 3, steps - 1, edge)
    comm(steps + CROSS)
    arrive(steps - 1)
    accumulate(steps - 1, 2, 0, rows)

    for f, o in ((0, out), (1, dout)):
        for r in range(rows):
            at = r * pair + f * width
            o[0, r] = (field[f, r + 1].astype(F32) + acc[at:at + width]).astype(BF16)

    def drain(s, carry):
        @pl.when(fetches(s))
        def _():
            for k in range(2):
                own_copy(s, k).wait_send()
            relay_copy(s).wait_send()

        @pl.when(jnp.logical_and(fetches(s), shared(s)))
        def _():
            for k in range(3):
                plane_copy(s, k).wait_send()

        for k in range(3):
            pair_copy(s, k).wait_send()
        return carry
    lax.fori_loop(0, steps, drain, 0)
    for k in range(2):
        for j in range(n - 1):
            stat_copy(k, j).wait_send()


def fused(n, latents, latent_tangent, gain_first, weight_first, gain_second, weight_second):
    rows, width, chans = latents.shape[1:]
    size = chans // GROUPS
    group = np.arange(chans) // size
    same_group = jnp.asarray(group[:, None] == group[None, :], BF16)
    vmem = pl.BlockSpec(memory_space=pltpu.VMEM)
    hbm = pl.BlockSpec(memory_space=pl.ANY)
    dma = pltpu.SemaphoreType.DMA
    steps = 2 * TAPS
    shape = jax.ShapeDtypeStruct(latents.shape, BF16)
    return pl.pallas_call(
        functools.partial(fused_kernel, n),
        out_shape=(shape, shape),
        in_specs=[hbm, hbm, vmem, vmem, hbm, hbm, vmem],
        out_specs=(vmem, vmem),
        scratch_shapes=[
            pltpu.VMEM((2, rows + 2, width, chans), BF16),
            pltpu.VMEM((2, rows + 2, width, chans), BF16),
            pltpu.VMEM((3, (rows + 2) * 2 * width, chans), BF16),
            pltpu.VMEM((2 * rows * width, chans), F32),
            pltpu.VMEM((steps, chans, chans), BF16),
            pltpu.VMEM((2, 8, chans), F32),
            pltpu.VMEM((2, n - 1, 8, chans), F32),
            dma((8,)),
            dma((2, 2, 2)),
            dma((2, 2, 2)),
            dma((2, n - 1)),
            dma((2, n - 1)),
            dma((steps, 2)),
            dma((steps, 2)),
            dma((steps,)),
            dma((steps,)),
            dma((steps, 3)),
            dma((steps, 3)),
            dma((steps, 3)),
            dma((steps, 3)),
        ],
        compiler_params=pltpu.CompilerParams(
            collective_id=0, has_side_effects=True, vmem_limit_bytes=60 * 1024 * 1024),
    )(
        latents, latent_tangent, gain_first, gain_second,
        weight_first.transpose(0, 2, 1), weight_second.transpose(0, 2, 1), same_group)


def extended(cells, sides, width):
    for axis, dim in sides:
        count = lax.axis_size(axis)
        ends = count - 1
        head = lax.slice_in_dim(cells, 0, width, axis=dim)
        tail = lax.slice_in_dim(cells, cells.shape[dim] - width, cells.shape[dim], axis=dim)
        cells = jnp.concatenate(
            [
                lax.ppermute(tail, axis, [(i, (i + 1) % count) for i in range(ends)]),
                cells,
                lax.ppermute(head, axis, [((i + 1) % count, i) for i in range(ends)]),
            ],
            axis=dim,
        )
    return cells


def normalize(stacked, gain_vector):
    row_count, col_count, chans = (stacked.shape[1], stacked.shape[2], stacked.shape[3])
    size = chans // GROUPS
    positions = float(row_count * col_count * size * lax.axis_size("height"))
    grouped = stacked.reshape(2, row_count * col_count, GROUPS, size)
    primal = grouped[0]
    tangent = grouped[1]
    first_totals = lax.psum((jnp.sum(primal, axis=(0, 2)), jnp.sum(tangent, axis=(0, 2))), "height")
    group_mean = first_totals[0] / positions
    tangent_mean = first_totals[1] / positions
    centered = primal - group_mean[None, :, None]
    tangent_centered = tangent - tangent_mean[None, :, None]
    second_totals = lax.psum(
        (
            jnp.sum(centered * centered, axis=(0, 2)),
            jnp.sum(centered * tangent_centered, axis=(0, 2)),
        ),
        "height",
    )
    variance = second_totals[0] / positions
    dvariance = 2.0 * second_totals[1] / positions
    inverse = lax.rsqrt(variance + epsilon)[None, :, None]
    normed = centered * inverse
    dnormed = tangent_centered * inverse - centered * (0.5 * dvariance[None, :, None] * inverse**3)
    scaled = normed.reshape(row_count, col_count, chans) * gain_vector
    dscaled = dnormed.reshape(row_count, col_count, chans) * gain_vector
    sigmoid_value = jax.nn.sigmoid(scaled)
    hidden = scaled * sigmoid_value
    dhidden = dscaled * sigmoid_value * (1.0 + scaled * (1.0 - sigmoid_value))
    return jnp.stack([hidden, dhidden], 0).astype(jnp.bfloat16)


def apply_taps(padded, weight_piece, row_count, col_count):
    chans = padded.shape[3]
    accumulated = jnp.zeros((2 * row_count * col_count, weight_piece.shape[2]), jnp.float32)
    for tap_index in range(9):
        offset_row = tap_index // 3
        offset_col = tap_index % 3
        window = padded[
            :, offset_row : offset_row + row_count, offset_col : offset_col + col_count, :
        ].reshape(-1, chans)
        accumulated = accumulated + jnp.dot(
            window, weight_piece[tap_index], preferred_element_type=jnp.float32
        )
    return accumulated


def convolve(hidden, weight):
    row_count, col_count = (hidden.shape[1], hidden.shape[2])
    padded = extended(hidden, (("height", 1),), 1)
    padded = jnp.pad(padded, ((0, 0), (0, 0), (1, 1), (0, 0)))
    flattened = apply_taps(
        padded, lax.all_gather(weight, "height", axis=2, tiled=True), row_count, col_count
    )
    return flattened.reshape(2, row_count, col_count, -1)


def per_device(latents, latent_tangent, gain_first, weight_first, gain_second, weight_second):
    stacked = jnp.concatenate([latents, latent_tangent], 0).astype(jnp.float32)
    hidden = normalize(stacked, gain_first)
    middle = convolve(hidden, weight_first).astype(jnp.bfloat16)
    second = normalize(middle.astype(jnp.float32), gain_second)
    result = (stacked + convolve(second, weight_second)).astype(jnp.bfloat16)
    return (result[0:1], result[1:2])


def solution(mesh):
    placed = (
        P("dp", "height", None, None),
        P("dp", "height", None, None),
        P(),
        P(None, None, "height"),
        P(),
        P(None, None, "height"),
    )
    n = mesh.shape["height"]
    body = per_device
    if n == 4 and mesh.shape["dp"] % 4 == 0:
        body = functools.partial(fused, n)
    return jax.shard_map(
        body,
        mesh=mesh,
        in_specs=placed,
        out_specs=(P("dp", "height", None, None), P("dp", "height", None, None)),
        check_vma=False,
    )
```

```python
import functools

import jax
import jax.numpy as jnp
import numpy as np
from jax import lax
from jax.experimental import pallas as pl
from jax.experimental.pallas import tpu as pltpu
from jax.sharding import PartitionSpec as P

GROUPS = 32
TAPS = 9
ALONE = 8
DOUBLE = 15
FIRST = 4
OWN = (7, 9, 12, 12, 14, 14, 14, 15, 16, 17, 17, 18, 18, 18, 18, 18, 18, 18, 18, 18, 18, 18, 18)
NEAR = (2, 5, 7, 9, 10, 10, 12, 12, 13, 13, 14, 15, 17, 17, 17, 17, 18, 18, 18, 18, 18, 18, 18)
LATE = (0, 2, 3, 7, 7, 9, 9, 10, 10, 10, 10, 10, 12, 14, 14, 15, 15, 16, 16, 17, 18, 18, 18)
CROSS = (0, 0, 1, 2, 3, 6, 6, 8, 8, 9, 9, 9, 10, 12, 12, 12, 14, 16, 16, 17, 17, 17, 18)

epsilon = 1e-05
F32 = jnp.float32
BF16 = jnp.bfloat16


def fused_kernel(
    n, lat, tan, gain_a, gain_b, weight_a, weight_b, same_group,
    out, dout,
    field, mid, shifted, acc, full, stat, peer_stat,
    load_sem, halo_send, halo_recv, stat_send, stat_recv,
    own_send, near_recv, relay_send, far_recv, pair_send, pair_recv,
    plane_send, plane_recv,
):
    rows, width, chans = lat.shape[1], lat.shape[2], lat.shape[3]
    quarter = chans // n
    half = quarter // 2
    steps = 2 * TAPS
    local = rows * width
    pair = 2 * width
    d = lax.axis_index("dp")
    h = lax.axis_index("height")
    core = lax.rem(d, 2)
    xor1 = h + 1 - 2 * lax.rem(h, 2)
    xor2 = lax.rem(h + 2, n)
    xor3 = xor1 + 2 - 4 * (xor1 // 2)
    other = d + 1 - 2 * core
    peers = (xor1, xor2, xor3)
    plane = lax.rem(d // 2, 2)
    across = d + 2 - 4 * plane

    def start_remote(src, dst, send, recv, dd, hh):
        return pltpu.make_async_remote_copy(
            src_ref=src, dst_ref=dst, send_sem=send, recv_sem=recv,
            device_id={"dp": dd, "height": hh},
            device_id_type=pl.DeviceIdType.MESH,
        )

    barrier = pltpu.get_barrier_semaphore()
    for hh in peers:
        pl.semaphore_signal(barrier, inc=1, device_id={"dp": d, "height": hh}, device_id_type=pl.DeviceIdType.MESH)
    pl.semaphore_signal(barrier, inc=1, device_id={"dp": other, "height": h}, device_id_type=pl.DeviceIdType.MESH)

    pl.semaphore_signal(barrier, inc=1, device_id={"dp": across, "height": h}, device_id_type=pl.DeviceIdType.MESH)

    loads = [
        pltpu.make_async_copy(lat.at[0], field.at[0, pl.ds(1, rows)], load_sem.at[0]),
        pltpu.make_async_copy(tan.at[0], field.at[1, pl.ds(1, rows)], load_sem.at[1]),
    ] + [
        pltpu.make_async_copy(
            w.at[pl.ds(3 * src, 3)],
            full.at[pl.ds(TAPS * i + 3 * dst, 3), pl.ds(pl.multiple_of(h * quarter, 16), quarter)],
            load_sem.at[2 + 3 * i + dst])
        for i, w in enumerate((weight_a, weight_b)) for dst, src in enumerate((1, 0, 2))
    ]
    for c in loads:
        c.start()
    def rows_of(hh, cc):
        return pl.ds(pl.multiple_of(hh * quarter + cc * half, 16), half)

    def shared(s):
        return s < ALONE or TAPS <= s < DOUBLE

    def fetched(s, side):
        return not shared(s) or s % TAPS % 2 == side

    corner = jnp.logical_or(h == 0, h == n - 1)
    turn_source = jnp.where(corner, xor2, xor1)
    turn_target = jnp.where(corner, xor1, xor2)

    def tap_of(v):
        part = lax.rem(v, TAPS)
        row = part // 3
        return 1 - row + 3 * (row // 2), lax.rem(part, 3)

    def own_copy(s, k, w=None, tap=None):
        if w is None:
            src = full.at[s, rows_of(h, core)]
        else:
            src = w.at[tap, pl.ds(pl.multiple_of(core * half, 16), half)]
        return start_remote(
            src, full.at[s, rows_of(h, core)],
            own_send.at[s, k], near_recv.at[s, k], d, peers[k])

    def relay_copy(s):
        turn = s % TAPS // 2 % 2 == 1
        block = full.at[s, rows_of(turn_source if turn else xor1, core)]
        return start_remote(block, block, relay_send.at[s], far_recv.at[s], d, turn_target if turn else xor2)

    def pair_copy(s, k):
        block = full.at[s, rows_of(peers[k], core)]
        return start_remote(block, block, pair_send.at[s, k], pair_recv.at[s, k], other, h)

    def plane_copy(s, k):
        block = full.at[s, rows_of(peers[k], core)]
        return start_remote(block, block, plane_send.at[s, k], plane_recv.at[s, k], across, h)

    def send_own(s, side):
        if fetched(s, side):
            p, q = (1, 0, 2)[s % TAPS // 3], s % 3
            for k in range(2):
                own_copy(s, k, (weight_a, weight_b)[s // TAPS], 3 * p + q).start()

    def pass_on(s, k):
        pair_copy(s, k).start()
        if shared(s):
            plane_copy(s, k).start()

    def relay(s, side):
        if fetched(s, side):
            for k in range(2):
                own_copy(s, k).wait_recv()
            relay_copy(s).start()
            for k in range(2):
                pass_on(s, k)

    def spread(s, side):
        if fetched(s, side):
            relay_copy(s).wait_recv()
            pass_on(s, 2)

    def mirror(s, side):
        if not fetched(s, side):
            for k in range(3):
                plane_copy(s, k).wait_recv()
                pair_copy(s, k).start()

    def both_planes(work):
        for side in range(2):
            @pl.when(plane == side)
            def _(side=side):
                for action, s in work:
                    action(s, side)

    def tick(t):
        work = []
        for action, table in ((spread, LATE), (mirror, CROSS), (relay, NEAR), (send_own, OWN)):
            before = table[t - 1] if t else FIRST if table is OWN else 0
            work += [(action, s) for s in range(before, table[t])]
        if work:
            both_planes(work)

    def loop(low, high, body):
        def one(v, carry):
            body(v)
            return carry
        lax.fori_loop(low, high, one, 0)

    def ticks(v, low, high, offset):
        for u in range(low, high):
            @pl.when(v == u)
            def _(u=u):
                tick(u + offset)

    def halo_copies(buf, k):
        top = [start_remote(buf.at[f, 1], buf.at[f, rows + 1], halo_send.at[k, 0, f], halo_recv.at[k, 0, f], d, lax.rem(h + n - 1, n)) for f in range(2)]
        low = [start_remote(buf.at[f, rows], buf.at[f, 0], halo_send.at[k, 1, f], halo_recv.at[k, 1, f], d, lax.rem(h + 1, n)) for f in range(2)]
        return top, low

    def halo_start(buf, k, sources=None, fields=(0, 1)):
        def edge_row(f, r):
            return buf.at[f, 1 + r] if sources is None else sources[f].at[0, r]

        @pl.when(h > 0)
        def _():
            for f in fields:
                start_remote(edge_row(f, 0), buf.at[f, rows + 1], halo_send.at[k, 0, f], halo_recv.at[k, 0, f], d, lax.rem(h + n - 1, n)).start()

        @pl.when(h < n - 1)
        def _():
            for f in fields:
                start_remote(edge_row(f, rows - 1), buf.at[f, 0], halo_send.at[k, 1, f], halo_recv.at[k, 1, f], d, lax.rem(h + 1, n)).start()

    def halo_wait(buf, k):
        top, low = halo_copies(buf, k)

        @pl.when(h > 0)
        def _():
            for c in top:
                c.wait_send()
            for c in low:
                c.wait_recv()

        @pl.when(h < n - 1)
        def _():
            for c in low:
                c.wait_send()
            for c in top:
                c.wait_recv()

    def local_stats(buf, k):
        zero = jnp.zeros((1, chans), F32)

        def sums(r, carry):
            return (
                carry[0] + jnp.sum(buf[0, r].astype(F32), axis=0, keepdims=True),
                carry[1] + jnp.sum(buf[1, r].astype(F32), axis=0, keepdims=True),
            )

        total, dtotal = lax.fori_loop(1, rows + 1, sums, (zero, zero))
        mean = total / local
        dmean = dtotal / local

        def moments(r, carry):
            v = buf[0, r].astype(F32) - mean
            dv = buf[1, r].astype(F32) - dmean
            return (
                carry[0] + jnp.sum(v * v, axis=0, keepdims=True),
                carry[1] + jnp.sum(v * dv, axis=0, keepdims=True),
            )

        second, dsecond = lax.fori_loop(1, rows + 1, moments, (zero, zero))
        stat[k, 0:1] = mean
        stat[k, 1:2] = dmean
        stat[k, 2:3] = second
        stat[k, 3:4] = dsecond
        stat[k, 4:8] = jnp.zeros((4, chans), F32)

    def stat_copy(k, j):
        return start_remote(stat.at[k], peer_stat.at[k, j], stat_send.at[k, j], stat_recv.at[k, j], d, peers[j])

    def group_sum(x):
        high = x.astype(BF16)
        rest = x - high.astype(F32)
        middle = rest.astype(BF16)
        low = (rest - middle.astype(F32)).astype(BF16)
        dot = lambda part: jnp.dot(part, same_group[...], preferred_element_type=F32)
        return dot(high) + dot(middle) + dot(low)

    def coefficients(k, gain):
        gain_row = gain[...].reshape(1, chans)
        for j in range(n - 1):
            stat_copy(k, j).wait_recv()
        size = chans // GROUPS
        blocks = [stat[k]] + [peer_stat[k, j] for j in range(n - 1)]
        both = blocks[0]
        for b in blocks[1:]:
            both = both + b
        means = group_sum(both) / (n * size)
        mean, dmean = means[0:1], means[1:2]
        var = jnp.zeros((1, chans), F32)
        dvar = jnp.zeros((1, chans), F32)
        for b in blocks:
            off = b[0:1] - mean
            doff = b[1:2] - dmean
            var = var + (b[2:3] + local * (off * off))
            dvar = dvar + (b[3:4] + local * (off * doff))
        row = lax.broadcasted_iota(jnp.int32, (8, chans), 0)
        packed = jnp.where(row == 0, var, jnp.where(row == 1, dvar, 0.0))
        moments = group_sum(packed) / (n * size * local)
        inverse = lax.rsqrt(moments[0:1] + epsilon)
        scale = gain_row * inverse
        slope = gain_row * (moments[1:2] * inverse * inverse * inverse)
        return mean, dmean, scale, slope

    column = lax.broadcasted_iota(jnp.int32, (width, 1), 0)

    def activate(buf, r, coef, keep):
        mean, dmean, scale, slope = coef
        v = buf[0, r].astype(F32) - mean
        dv = buf[1, r].astype(F32) - dmean
        a = v * scale
        da = dv * scale - v * slope
        s = jax.nn.sigmoid(a)
        hid = a * s
        dhid = da * (s * (1.0 + a * (1.0 - s)))
        if keep is not None:
            hid = jnp.where(keep, hid, 0.0)
            dhid = jnp.where(keep, dhid, 0.0)
        for f, x in ((0, hid), (1, dhid)):
            at = pl.ds(pl.multiple_of(r * pair + f * width, 128), width)
            shifted[1, at] = x.astype(BF16)
            shifted[0, at] = jnp.where(column == 0, 0.0, pltpu.roll(x, 1, 0)).astype(BF16)
            shifted[2, at] = jnp.where(column == width - 1, 0.0, pltpu.roll(x, width - 1, 0)).astype(BF16)

    def activate_rows(buf, coef):
        def one(r, carry):
            activate(buf, r, coef, None)
            return carry
        lax.fori_loop(1, rows + 1, one, 0)

    def activate_halo(buf, coef):
        def one(e, carry):
            r = e * (rows + 1)
            edge = jnp.where(e == 0, 0, n - 1)
            activate(buf, r, coef, h != edge)
            return carry
        lax.fori_loop(0, 2, one, 0)

    def arrive(v):
        for k in range(3):
            pair_copy(v, k).wait_recv()

    def accumulate(v, src, dst, count):
        q = tap_of(v)[1]
        at = pl.ds(pl.multiple_of(dst * pair, 128), count * pair)
        acc[at] += lax.dot_general(
            shifted[q, pl.ds(pl.multiple_of(src * pair, 128), count * pair)], full[v],
            (((1,), (1,)), ((), ())), preferred_element_type=F32)

    def center(low, high, offset):
        def one(v):
            ticks(v, low, high, offset)
            arrive(v)
            accumulate(v, 1, 0, rows)
        loop(low, high, one)

    def inner(low, high, offset):
        def one(v):
            ticks(v, low, high, offset)
            arrive(v)
            p = tap_of(v)[0]
            accumulate(v, 1 + p // 2, 1 - p // 2, rows - 1)
        loop(low, high, one)

    def edge(v):
        p = tap_of(v)[0]
        accumulate(v, (p // 2) * (rows + 1), (p // 2) * (rows - 1), 1)

    loads[0].wait()
    loads[1].wait()
    local_stats(field, 0)
    pl.semaphore_wait(barrier, n + 1)
    for j in range(n - 1):
        stat_copy(0, j).start()
    both_planes([(send_own, s) for s in range(FIRST)])
    tick(0)
    halo_start(field, 0, (lat, tan), (0,))
    acc[...] = jnp.zeros_like(acc)
    coef = coefficients(0, gain_a)
    tick(1)
    activate_rows(field, coef)
    for c in loads[2:5]:
        c.wait()
    center(0, 2, 2)
    halo_start(field, 0, (lat, tan), (1,))
    center(2, 3, 2)
    inner(3, 9, 2)
    tick(11)
    halo_wait(field, 0)
    activate_halo(field, coef)
    loop(3, TAPS, edge)

    for c in loads[5:]:
        c.wait()
    for f in range(2):
        for r in range(rows):
            at = r * pair + f * width
            mid[f, r + 1] = acc[at:at + width].astype(BF16)
    local_stats(mid, 1)
    for j in range(n - 1):
        stat_copy(1, j).start()
    halo_start(mid, 1)
    tick(12)
    acc[...] = jnp.zeros_like(acc)
    coef = coefficients(1, gain_b)
    tick(13)
    activate_rows(mid, coef)
    center(TAPS, TAPS + 3, 5)
    inner(TAPS + 3, 17, 5)
    halo_wait(mid, 1)
    activate_halo(mid, coef)
    loop(TAPS + 3, 17, edge)
    tick(22)
    arrive(steps - 1)
    accumulate(steps - 1, 2, 0, rows)

    for f, o in ((0, out), (1, dout)):
        for r in range(rows):
            at = r * pair + f * width
            o[0, r] = (field[f, r + 1].astype(F32) + acc[at:at + width]).astype(BF16)

    def drain(s, side):
        if fetched(s, side):
            for k in range(2):
                own_copy(s, k).wait_send()
            relay_copy(s).wait_send()
            if shared(s):
                for k in range(3):
                    plane_copy(s, k).wait_send()
        for k in range(3):
            pair_copy(s, k).wait_send()
    both_planes([(drain, s) for s in range(steps)])
    for k in range(2):
        for j in range(n - 1):
            stat_copy(k, j).wait_send()


def fused(n, latents, latent_tangent, gain_first, weight_first, gain_second, weight_second):
    rows, width, chans = latents.shape[1:]
    size = chans // GROUPS
    group = np.arange(chans) // size
    same_group = jnp.asarray(group[:, None] == group[None, :], BF16)
    vmem = pl.BlockSpec(memory_space=pltpu.VMEM)
    hbm = pl.BlockSpec(memory_space=pl.ANY)
    dma = pltpu.SemaphoreType.DMA
    steps = 2 * TAPS
    shape = jax.ShapeDtypeStruct(latents.shape, BF16)
    return pl.pallas_call(
        functools.partial(fused_kernel, n),
        out_shape=(shape, shape),
        in_specs=[hbm, hbm, vmem, vmem, hbm, hbm, vmem],
        out_specs=(vmem, vmem),
        scratch_shapes=[
            pltpu.VMEM((2, rows + 2, width, chans), BF16),
            pltpu.VMEM((2, rows + 2, width, chans), BF16),
            pltpu.VMEM((3, (rows + 2) * 2 * width, chans), BF16),
            pltpu.VMEM((2 * rows * width, chans), F32),
            pltpu.VMEM((steps, chans, chans), BF16),
            pltpu.VMEM((2, 8, chans), F32),
            pltpu.VMEM((2, n - 1, 8, chans), F32),
            dma((8,)),
            dma((2, 2, 2)),
            dma((2, 2, 2)),
            dma((2, n - 1)),
            dma((2, n - 1)),
            dma((steps, 2)),
            dma((steps, 2)),
            dma((steps,)),
            dma((steps,)),
            dma((steps, 3)),
            dma((steps, 3)),
            dma((steps, 3)),
            dma((steps, 3)),
        ],
        compiler_params=pltpu.CompilerParams(
            collective_id=0, has_side_effects=True, vmem_limit_bytes=60 * 1024 * 1024),
    )(
        latents, latent_tangent, gain_first, gain_second,
        weight_first.transpose(0, 2, 1), weight_second.transpose(0, 2, 1), same_group)


def extended(cells, sides, width):
    for axis, dim in sides:
        count = lax.axis_size(axis)
        ends = count - 1
        head = lax.slice_in_dim(cells, 0, width, axis=dim)
        tail = lax.slice_in_dim(cells, cells.shape[dim] - width, cells.shape[dim], axis=dim)
        cells = jnp.concatenate(
            [
                lax.ppermute(tail, axis, [(i, (i + 1) % count) for i in range(ends)]),
                cells,
                lax.ppermute(head, axis, [((i + 1) % count, i) for i in range(ends)]),
            ],
            axis=dim,
        )
    return cells


def normalize(stacked, gain_vector):
    row_count, col_count, chans = (stacked.shape[1], stacked.shape[2], stacked.shape[3])
    size = chans // GROUPS
    positions = float(row_count * col_count * size * lax.axis_size("height"))
    grouped = stacked.reshape(2, row_count * col_count, GROUPS, size)
    primal = grouped[0]
    tangent = grouped[1]
    first_totals = lax.psum((jnp.sum(primal, axis=(0, 2)), jnp.sum(tangent, axis=(0, 2))), "height")
    group_mean = first_totals[0] / positions
    tangent_mean = first_totals[1] / positions
    centered = primal - group_mean[None, :, None]
    tangent_centered = tangent - tangent_mean[None, :, None]
    second_totals = lax.psum(
        (
            jnp.sum(centered * centered, axis=(0, 2)),
            jnp.sum(centered * tangent_centered, axis=(0, 2)),
        ),
        "height",
    )
    variance = second_totals[0] / positions
    dvariance = 2.0 * second_totals[1] / positions
    inverse = lax.rsqrt(variance + epsilon)[None, :, None]
    normed = centered * inverse
    dnormed = tangent_centered * inverse - centered * (0.5 * dvariance[None, :, None] * inverse**3)
    scaled = normed.reshape(row_count, col_count, chans) * gain_vector
    dscaled = dnormed.reshape(row_count, col_count, chans) * gain_vector
    sigmoid_value = jax.nn.sigmoid(scaled)
    hidden = scaled * sigmoid_value
    dhidden = dscaled * sigmoid_value * (1.0 + scaled * (1.0 - sigmoid_value))
    return jnp.stack([hidden, dhidden], 0).astype(jnp.bfloat16)


def apply_taps(padded, weight_piece, row_count, col_count):
    chans = padded.shape[3]
    accumulated = jnp.zeros((2 * row_count * col_count, weight_piece.shape[2]), jnp.float32)
    for tap_index in range(9):
        offset_row = tap_index // 3
        offset_col = tap_index % 3
        window = padded[
            :, offset_row : offset_row + row_count, offset_col : offset_col + col_count, :
        ].reshape(-1, chans)
        accumulated = accumulated + jnp.dot(
            window, weight_piece[tap_index], preferred_element_type=jnp.float32
        )
    return accumulated


def convolve(hidden, weight):
    row_count, col_count = (hidden.shape[1], hidden.shape[2])
    padded = extended(hidden, (("height", 1),), 1)
    padded = jnp.pad(padded, ((0, 0), (0, 0), (1, 1), (0, 0)))
    flattened = apply_taps(
        padded, lax.all_gather(weight, "height", axis=2, tiled=True), row_count, col_count
    )
    return flattened.reshape(2, row_count, col_count, -1)


def per_device(latents, latent_tangent, gain_first, weight_first, gain_second, weight_second):
    stacked = jnp.concatenate([latents, latent_tangent], 0).astype(jnp.float32)
    hidden = normalize(stacked, gain_first)
    middle = convolve(hidden, weight_first).astype(jnp.bfloat16)
    second = normalize(middle.astype(jnp.float32), gain_second)
    result = (stacked + convolve(second, weight_second)).astype(jnp.bfloat16)
    return (result[0:1], result[1:2])


def solution(mesh):
    placed = (
        P("dp", "height", None, None),
        P("dp", "height", None, None),
        P(),
        P(None, None, "height"),
        P(),
        P(None, None, "height"),
    )
    n = mesh.shape["height"]
    body = per_device
    if n == 4 and mesh.shape["dp"] % 4 == 0:
        body = functools.partial(fused, n)
    return jax.shard_map(
        body,
        mesh=mesh,
        in_specs=placed,
        out_specs=(P("dp", "height", None, None), P("dp", "height", None, None)),
        check_vma=False,
    )
```

```python
import functools

import jax
import jax.numpy as jnp
import numpy as np
from jax import lax
from jax.experimental import pallas as pl
from jax.experimental.pallas import tpu as pltpu
from jax.sharding import PartitionSpec as P

GROUPS = 32
TAPS = 9
SHARED = (1, 1, 1, 0, 1, 1, 1, 0, 1, 1, 1, 1, 1, 1, 0, 1, 1, 0)
SIDE = (0, 0, 1, 0, 1, 0, 1, 0, 1, 0, 0, 1, 0, 1, 1, 1, 0, 1)
TURN = (1, 0, 1, 1, 0, 1, 0, 0, 1, 0, 1, 1, 1, 1, 1, 1, 1, 1)
FIRST = 7
OWN = (10, 11, 13, 14, 14, 14, 14, 14, 16, 18, 18, 18, 18, 18, 18, 18, 18, 18, 18, 18, 18, 18, 18)
NEAR = (2, 7, 9, 9, 11, 11, 11, 12, 12, 12, 12, 14, 18, 18, 18, 18, 18, 18, 18, 18, 18, 18, 18)
LATE = (0, 2, 4, 5, 7, 8, 9, 9, 9, 9, 10, 11, 14, 14, 14, 15, 17, 17, 17, 17, 18, 18, 18)
CROSS = (0, 0, 1, 4, 4, 5, 5, 7, 9, 9, 9, 9, 10, 11, 12, 14, 14, 15, 15, 18, 18, 18, 18)

epsilon = 1e-05
F32 = jnp.float32
BF16 = jnp.bfloat16


def fused_kernel(
    n, lat, tan, gain_a, gain_b, weight_a, weight_b, same_group,
    out, dout,
    field, mid, shifted, acc, full, stat, peer_stat,
    load_sem, halo_send, halo_recv, stat_send, stat_recv,
    own_send, near_recv, relay_send, far_recv, pair_send, pair_recv,
    plane_send, plane_recv,
):
    rows, width, chans = lat.shape[1], lat.shape[2], lat.shape[3]
    quarter = chans // n
    half = quarter // 2
    steps = 2 * TAPS
    local = rows * width
    pair = 2 * width
    d = lax.axis_index("dp")
    h = lax.axis_index("height")
    core = lax.rem(d, 2)
    xor1 = h + 1 - 2 * lax.rem(h, 2)
    xor2 = lax.rem(h + 2, n)
    xor3 = xor1 + 2 - 4 * (xor1 // 2)
    other = d + 1 - 2 * core
    peers = (xor1, xor2, xor3)
    plane = lax.rem(d // 2, 2)
    across = d + 2 - 4 * plane

    def start_remote(src, dst, send, recv, dd, hh):
        return pltpu.make_async_remote_copy(
            src_ref=src, dst_ref=dst, send_sem=send, recv_sem=recv,
            device_id={"dp": dd, "height": hh},
            device_id_type=pl.DeviceIdType.MESH,
        )

    barrier = pltpu.get_barrier_semaphore()
    for hh in peers:
        pl.semaphore_signal(barrier, inc=1, device_id={"dp": d, "height": hh}, device_id_type=pl.DeviceIdType.MESH)
    pl.semaphore_signal(barrier, inc=1, device_id={"dp": other, "height": h}, device_id_type=pl.DeviceIdType.MESH)

    pl.semaphore_signal(barrier, inc=1, device_id={"dp": across, "height": h}, device_id_type=pl.DeviceIdType.MESH)

    loads = [
        pltpu.make_async_copy(lat.at[0], field.at[0, pl.ds(1, rows)], load_sem.at[0]),
        pltpu.make_async_copy(tan.at[0], field.at[1, pl.ds(1, rows)], load_sem.at[1]),
    ] + [
        pltpu.make_async_copy(
            w.at[pl.ds(3 * src, 3)],
            full.at[pl.ds(TAPS * i + 3 * dst, 3), pl.ds(pl.multiple_of(h * quarter, 16), quarter)],
            load_sem.at[2 + 3 * i + dst])
        for i, w in enumerate((weight_a, weight_b)) for dst, src in enumerate((1, 0, 2))
    ]
    for c in loads:
        c.start()
    def rows_of(hh, cc):
        return pl.ds(pl.multiple_of(hh * quarter + cc * half, 16), half)

    def shared(s):
        return SHARED[s] == 1

    def fetched(s, side):
        return not shared(s) or SIDE[s] == side

    corner = jnp.logical_or(h == 0, h == n - 1)
    turn_source = jnp.where(corner, xor2, xor1)
    turn_target = jnp.where(corner, xor1, xor2)

    def tap_of(v):
        part = lax.rem(v, TAPS)
        row = part // 3
        return 1 - row + 3 * (row // 2), lax.rem(part, 3)

    def own_copy(s, k, w=None, tap=None):
        if w is None:
            src = full.at[s, rows_of(h, core)]
        else:
            src = w.at[tap, pl.ds(pl.multiple_of(core * half, 16), half)]
        return start_remote(
            src, full.at[s, rows_of(h, core)],
            own_send.at[s, k], near_recv.at[s, k], d, peers[k])

    def relay_copy(s):
        turn = TURN[s] == 1
        block = full.at[s, rows_of(turn_source if turn else xor1, core)]
        return start_remote(block, block, relay_send.at[s], far_recv.at[s], d, turn_target if turn else xor2)

    def pair_copy(s, k):
        block = full.at[s, rows_of(peers[k], core)]
        return start_remote(block, block, pair_send.at[s, k], pair_recv.at[s, k], other, h)

    def plane_copy(s, k):
        block = full.at[s, rows_of(peers[k], core)]
        return start_remote(block, block, plane_send.at[s, k], plane_recv.at[s, k], across, h)

    def send_own(s, side):
        if fetched(s, side):
            p, q = (1, 0, 2)[s % TAPS // 3], s % 3
            for k in range(2):
                own_copy(s, k, (weight_a, weight_b)[s // TAPS], 3 * p + q).start()

    def pass_on(s, k):
        pair_copy(s, k).start()
        if shared(s):
            plane_copy(s, k).start()

    def relay(s, side):
        if fetched(s, side):
            for k in range(2):
                own_copy(s, k).wait_recv()
            relay_copy(s).start()
            for k in range(2):
                pass_on(s, k)

    def spread(s, side):
        if fetched(s, side):
            relay_copy(s).wait_recv()
            pass_on(s, 2)

    def mirror(s, side):
        if not fetched(s, side):
            for k in range(3):
                plane_copy(s, k).wait_recv()
                pair_copy(s, k).start()

    def both_planes(work):
        for side in range(2):
            @pl.when(plane == side)
            def _(side=side):
                for action, s in work:
                    action(s, side)

    def tick(t):
        work = []
        for action, table in ((mirror, CROSS), (spread, LATE), (relay, NEAR), (send_own, OWN)):
            before = table[t - 1] if t else FIRST if table is OWN else 0
            work += [(action, s) for s in range(before, table[t])]
        if work:
            both_planes(work)

    def loop(low, high, body):
        def one(v, carry):
            body(v)
            return carry
        lax.fori_loop(low, high, one, 0)

    def ticks(v, low, high, offset):
        for u in range(low, high):
            @pl.when(v == u)
            def _(u=u):
                tick(u + offset)

    def halo_copies(buf, k):
        top = [start_remote(buf.at[f, 1], buf.at[f, rows + 1], halo_send.at[k, 0, f], halo_recv.at[k, 0, f], d, lax.rem(h + n - 1, n)) for f in range(2)]
        low = [start_remote(buf.at[f, rows], buf.at[f, 0], halo_send.at[k, 1, f], halo_recv.at[k, 1, f], d, lax.rem(h + 1, n)) for f in range(2)]
        return top, low

    def halo_start(buf, k, sources=None, fields=(0, 1)):
        def edge_row(f, r):
            return buf.at[f, 1 + r] if sources is None else sources[f].at[0, r]

        @pl.when(h > 0)
        def _():
            for f in fields:
                start_remote(edge_row(f, 0), buf.at[f, rows + 1], halo_send.at[k, 0, f], halo_recv.at[k, 0, f], d, lax.rem(h + n - 1, n)).start()

        @pl.when(h < n - 1)
        def _():
            for f in fields:
                start_remote(edge_row(f, rows - 1), buf.at[f, 0], halo_send.at[k, 1, f], halo_recv.at[k, 1, f], d, lax.rem(h + 1, n)).start()

    def halo_wait(buf, k):
        top, low = halo_copies(buf, k)

        @pl.when(h > 0)
        def _():
            for c in top:
                c.wait_send()
            for c in low:
                c.wait_recv()

        @pl.when(h < n - 1)
        def _():
            for c in low:
                c.wait_send()
            for c in top:
                c.wait_recv()

    def local_stats(buf, k):
        zero = jnp.zeros((1, chans), F32)

        def sums(r, carry):
            return (
                carry[0] + jnp.sum(buf[0, r].astype(F32), axis=0, keepdims=True),
                carry[1] + jnp.sum(buf[1, r].astype(F32), axis=0, keepdims=True),
            )

        total, dtotal = lax.fori_loop(1, rows + 1, sums, (zero, zero))
        mean = total / local
        dmean = dtotal / local

        def moments(r, carry):
            v = buf[0, r].astype(F32) - mean
            dv = buf[1, r].astype(F32) - dmean
            return (
                carry[0] + jnp.sum(v * v, axis=0, keepdims=True),
                carry[1] + jnp.sum(v * dv, axis=0, keepdims=True),
            )

        second, dsecond = lax.fori_loop(1, rows + 1, moments, (zero, zero))
        stat[k, 0:1] = mean
        stat[k, 1:2] = dmean
        stat[k, 2:3] = second
        stat[k, 3:4] = dsecond
        stat[k, 4:8] = jnp.zeros((4, chans), F32)

    def stat_copy(k, j):
        return start_remote(stat.at[k], peer_stat.at[k, j], stat_send.at[k, j], stat_recv.at[k, j], d, peers[j])

    def group_sum(x):
        high = x.astype(BF16)
        rest = x - high.astype(F32)
        middle = rest.astype(BF16)
        low = (rest - middle.astype(F32)).astype(BF16)
        dot = lambda part: jnp.dot(part, same_group[...], preferred_element_type=F32)
        return dot(high) + dot(middle) + dot(low)

    def coefficients(k, gain):
        gain_row = gain[...].reshape(1, chans)
        for j in range(n - 1):
            stat_copy(k, j).wait_recv()
        size = chans // GROUPS
        blocks = [stat[k]] + [peer_stat[k, j] for j in range(n - 1)]
        both = blocks[0]
        for b in blocks[1:]:
            both = both + b
        means = group_sum(both) / (n * size)
        mean, dmean = means[0:1], means[1:2]
        var = jnp.zeros((1, chans), F32)
        dvar = jnp.zeros((1, chans), F32)
        for b in blocks:
            off = b[0:1] - mean
            doff = b[1:2] - dmean
            var = var + (b[2:3] + local * (off * off))
            dvar = dvar + (b[3:4] + local * (off * doff))
        row = lax.broadcasted_iota(jnp.int32, (8, chans), 0)
        packed = jnp.where(row == 0, var, jnp.where(row == 1, dvar, 0.0))
        moments = group_sum(packed) / (n * size * local)
        inverse = lax.rsqrt(moments[0:1] + epsilon)
        scale = gain_row * inverse
        slope = gain_row * (moments[1:2] * inverse * inverse * inverse)
        return mean, dmean, scale, slope

    column = lax.broadcasted_iota(jnp.int32, (width, 1), 0)

    def activate(buf, r, coef, keep):
        mean, dmean, scale, slope = coef
        v = buf[0, r].astype(F32) - mean
        dv = buf[1, r].astype(F32) - dmean
        a = v * scale
        da = dv * scale - v * slope
        s = jax.nn.sigmoid(a)
        hid = a * s
        dhid = da * (s * (1.0 + a * (1.0 - s)))
        if keep is not None:
            hid = jnp.where(keep, hid, 0.0)
            dhid = jnp.where(keep, dhid, 0.0)
        for f, x in ((0, hid), (1, dhid)):
            at = pl.ds(pl.multiple_of(r * pair + f * width, 128), width)
            shifted[1, at] = x.astype(BF16)
            shifted[0, at] = jnp.where(column == 0, 0.0, pltpu.roll(x, 1, 0)).astype(BF16)
            shifted[2, at] = jnp.where(column == width - 1, 0.0, pltpu.roll(x, width - 1, 0)).astype(BF16)

    def activate_rows(buf, coef):
        def one(r, carry):
            activate(buf, r, coef, None)
            return carry
        lax.fori_loop(1, rows + 1, one, 0)

    def activate_halo(buf, coef):
        def one(e, carry):
            r = e * (rows + 1)
            edge = jnp.where(e == 0, 0, n - 1)
            activate(buf, r, coef, h != edge)
            return carry
        lax.fori_loop(0, 2, one, 0)

    def arrive(v):
        for k in range(3):
            pair_copy(v, k).wait_recv()

    def accumulate(v, src, dst, count):
        q = tap_of(v)[1]
        at = pl.ds(pl.multiple_of(dst * pair, 128), count * pair)
        acc[at] += lax.dot_general(
            shifted[q, pl.ds(pl.multiple_of(src * pair, 128), count * pair)], full[v],
            (((1,), (1,)), ((), ())), preferred_element_type=F32)

    def center(low, high, offset):
        def one(v):
            ticks(v, low, high, offset)
            arrive(v)
            accumulate(v, 1, 0, rows)
        loop(low, high, one)

    def inner(low, high, offset):
        def one(v):
            ticks(v, low, high, offset)
            arrive(v)
            p = tap_of(v)[0]
            accumulate(v, 1 + p // 2, 1 - p // 2, rows - 1)
        loop(low, high, one)

    def edge(v):
        p = tap_of(v)[0]
        accumulate(v, (p // 2) * (rows + 1), (p // 2) * (rows - 1), 1)

    loads[0].wait()
    loads[1].wait()
    local_stats(field, 0)
    pl.semaphore_wait(barrier, n + 1)
    for j in range(n - 1):
        stat_copy(0, j).start()
    both_planes([(send_own, s) for s in range(FIRST)])
    tick(0)
    acc[...] = jnp.zeros_like(acc)
    coef = coefficients(0, gain_a)
    tick(1)
    halo_start(field, 0, (lat, tan), (0,))
    activate_rows(field, coef)
    for c in loads[2:5]:
        c.wait()
    center(0, 1, 2)
    halo_start(field, 0, (lat, tan), (1,))
    center(1, 3, 2)
    inner(3, 9, 2)
    tick(11)
    halo_wait(field, 0)
    activate_halo(field, coef)
    loop(3, TAPS, edge)

    for c in loads[5:]:
        c.wait()
    for f in range(2):
        for r in range(rows):
            at = r * pair + f * width
            mid[f, r + 1] = acc[at:at + width].astype(BF16)
    local_stats(mid, 1)
    for j in range(n - 1):
        stat_copy(1, j).start()
    tick(12)
    halo_start(mid, 1, None, (0,))
    acc[...] = jnp.zeros_like(acc)
    coef = coefficients(1, gain_b)
    tick(13)
    halo_start(mid, 1, None, (1,))
    activate_rows(mid, coef)
    center(TAPS, TAPS + 3, 5)
    inner(TAPS + 3, 17, 5)
    halo_wait(mid, 1)
    activate_halo(mid, coef)
    loop(TAPS + 3, 17, edge)
    tick(22)
    arrive(steps - 1)
    accumulate(steps - 1, 2, 0, rows)

    for f, o in ((0, out), (1, dout)):
        for r in range(rows):
            at = r * pair + f * width
            o[0, r] = (field[f, r + 1].astype(F32) + acc[at:at + width]).astype(BF16)

    def drain(s, side):
        if fetched(s, side):
            for k in range(2):
                own_copy(s, k).wait_send()
            relay_copy(s).wait_send()
            if shared(s):
                for k in range(3):
                    plane_copy(s, k).wait_send()
        for k in range(3):
            pair_copy(s, k).wait_send()
    both_planes([(drain, s) for s in range(steps)])
    for k in range(2):
        for j in range(n - 1):
            stat_copy(k, j).wait_send()


def fused(n, latents, latent_tangent, gain_first, weight_first, gain_second, weight_second):
    rows, width, chans = latents.shape[1:]
    size = chans // GROUPS
    group = np.arange(chans) // size
    same_group = jnp.asarray(group[:, None] == group[None, :], BF16)
    vmem = pl.BlockSpec(memory_space=pltpu.VMEM)
    hbm = pl.BlockSpec(memory_space=pl.ANY)
    dma = pltpu.SemaphoreType.DMA
    steps = 2 * TAPS
    shape = jax.ShapeDtypeStruct(latents.shape, BF16)
    return pl.pallas_call(
        functools.partial(fused_kernel, n),
        out_shape=(pltpu.VMEM(latents.shape, BF16), pltpu.VMEM(latents.shape, BF16)),
        in_specs=[hbm, hbm, vmem, vmem, hbm, hbm, vmem],
        out_specs=(vmem, vmem),
        scratch_shapes=[
            pltpu.VMEM((2, rows + 2, width, chans), BF16),
            pltpu.VMEM((2, rows + 2, width, chans), BF16),
            pltpu.VMEM((3, (rows + 2) * 2 * width, chans), BF16),
            pltpu.VMEM((2 * rows * width, chans), F32),
            pltpu.VMEM((steps, chans, chans), BF16),
            pltpu.VMEM((2, 8, chans), F32),
            pltpu.VMEM((2, n - 1, 8, chans), F32),
            dma((8,)),
            dma((2, 2, 2)),
            dma((2, 2, 2)),
            dma((2, n - 1)),
            dma((2, n - 1)),
            dma((steps, 2)),
            dma((steps, 2)),
            dma((steps,)),
            dma((steps,)),
            dma((steps, 3)),
            dma((steps, 3)),
            dma((steps, 3)),
            dma((steps, 3)),
        ],
        compiler_params=pltpu.CompilerParams(
            collective_id=0, has_side_effects=True, vmem_limit_bytes=61 * 1024 * 1024),
    )(
        latents, latent_tangent, gain_first, gain_second,
        weight_first.transpose(0, 2, 1), weight_second.transpose(0, 2, 1), same_group)


def extended(cells, sides, width):
    for axis, dim in sides:
        count = lax.axis_size(axis)
        ends = count - 1
        head = lax.slice_in_dim(cells, 0, width, axis=dim)
        tail = lax.slice_in_dim(cells, cells.shape[dim] - width, cells.shape[dim], axis=dim)
        cells = jnp.concatenate(
            [
                lax.ppermute(tail, axis, [(i, (i + 1) % count) for i in range(ends)]),
                cells,
                lax.ppermute(head, axis, [((i + 1) % count, i) for i in range(ends)]),
            ],
            axis=dim,
        )
    return cells


def normalize(stacked, gain_vector):
    row_count, col_count, chans = (stacked.shape[1], stacked.shape[2], stacked.shape[3])
    size = chans // GROUPS
    positions = float(row_count * col_count * size * lax.axis_size("height"))
    grouped = stacked.reshape(2, row_count * col_count, GROUPS, size)
    primal = grouped[0]
    tangent = grouped[1]
    first_totals = lax.psum((jnp.sum(primal, axis=(0, 2)), jnp.sum(tangent, axis=(0, 2))), "height")
    group_mean = first_totals[0] / positions
    tangent_mean = first_totals[1] / positions
    centered = primal - group_mean[None, :, None]
    tangent_centered = tangent - tangent_mean[None, :, None]
    second_totals = lax.psum(
        (
            jnp.sum(centered * centered, axis=(0, 2)),
            jnp.sum(centered * tangent_centered, axis=(0, 2)),
        ),
        "height",
    )
    variance = second_totals[0] / positions
    dvariance = 2.0 * second_totals[1] / positions
    inverse = lax.rsqrt(variance + epsilon)[None, :, None]
    normed = centered * inverse
    dnormed = tangent_centered * inverse - centered * (0.5 * dvariance[None, :, None] * inverse**3)
    scaled = normed.reshape(row_count, col_count, chans) * gain_vector
    dscaled = dnormed.reshape(row_count, col_count, chans) * gain_vector
    sigmoid_value = jax.nn.sigmoid(scaled)
    hidden = scaled * sigmoid_value
    dhidden = dscaled * sigmoid_value * (1.0 + scaled * (1.0 - sigmoid_value))
    return jnp.stack([hidden, dhidden], 0).astype(jnp.bfloat16)


def apply_taps(padded, weight_piece, row_count, col_count):
    chans = padded.shape[3]
    accumulated = jnp.zeros((2 * row_count * col_count, weight_piece.shape[2]), jnp.float32)
    for tap_index in range(9):
        offset_row = tap_index // 3
        offset_col = tap_index % 3
        window = padded[
            :, offset_row : offset_row + row_count, offset_col : offset_col + col_count, :
        ].reshape(-1, chans)
        accumulated = accumulated + jnp.dot(
            window, weight_piece[tap_index], preferred_element_type=jnp.float32
        )
    return accumulated


def convolve(hidden, weight):
    row_count, col_count = (hidden.shape[1], hidden.shape[2])
    padded = extended(hidden, (("height", 1),), 1)
    padded = jnp.pad(padded, ((0, 0), (0, 0), (1, 1), (0, 0)))
    flattened = apply_taps(
        padded, lax.all_gather(weight, "height", axis=2, tiled=True), row_count, col_count
    )
    return flattened.reshape(2, row_count, col_count, -1)


def per_device(latents, latent_tangent, gain_first, weight_first, gain_second, weight_second):
    stacked = jnp.concatenate([latents, latent_tangent], 0).astype(jnp.float32)
    hidden = normalize(stacked, gain_first)
    middle = convolve(hidden, weight_first).astype(jnp.bfloat16)
    second = normalize(middle.astype(jnp.float32), gain_second)
    result = (stacked + convolve(second, weight_second)).astype(jnp.bfloat16)
    return (result[0:1], result[1:2])


def solution(mesh):
    placed = (
        P("dp", "height", None, None),
        P("dp", "height", None, None),
        P(),
        P(None, None, "height"),
        P(),
        P(None, None, "height"),
    )
    n = mesh.shape["height"]
    body = per_device
    if n == 4 and mesh.shape["dp"] % 4 == 0:
        body = functools.partial(fused, n)
    return jax.shard_map(
        body,
        mesh=mesh,
        in_specs=placed,
        out_specs=(P("dp", "height", None, None), P("dp", "height", None, None)),
        check_vma=False,
    )
```

```python
import functools

import jax
import jax.numpy as jnp
import numpy as np
from jax import lax
from jax.experimental import pallas as pl
from jax.experimental.pallas import tpu as pltpu
from jax.sharding import PartitionSpec as P

GROUPS = 32
TAPS = 9
SHARED = (1, 1, 1, 0, 1, 1, 1, 0, 1, 1, 1, 1, 1, 1, 0, 1, 1, 0)
SIDE = (0, 0, 1, 0, 1, 0, 1, 0, 1, 0, 0, 1, 0, 1, 1, 1, 0, 1)
TURN = (1, 0, 1, 1, 0, 1, 0, 0, 1, 0, 1, 1, 1, 1, 1, 1, 1, 1)
FIRST = 7
OWN = (10, 11, 13, 14, 14, 14, 14, 14, 16, 18, 18, 18, 18, 18, 18, 18, 18, 18, 18, 18, 18, 18, 18)
NEAR = (2, 7, 9, 9, 11, 11, 11, 12, 12, 12, 12, 14, 18, 18, 18, 18, 18, 18, 18, 18, 18, 18, 18)
LATE = (0, 2, 4, 5, 7, 8, 9, 9, 9, 9, 10, 11, 14, 14, 14, 15, 17, 17, 17, 17, 18, 18, 18)
CROSS = (0, 0, 1, 4, 4, 5, 5, 7, 9, 9, 9, 9, 10, 11, 12, 14, 14, 15, 15, 18, 18, 18, 18)

epsilon = 1e-05
F32 = jnp.float32
BF16 = jnp.bfloat16


def fused_kernel(
    n, lat, tan, gain_a, gain_b, weight_a, weight_b, same_group,
    out, dout,
    field, mid, shifted, acc, full, stat, peer_stat,
    load_sem, halo_send, halo_recv, stat_send, stat_recv,
    own_send, near_recv, relay_send, far_recv, pair_send, pair_recv,
    plane_send, plane_recv,
):
    rows, width, chans = lat.shape[1], lat.shape[2], lat.shape[3]
    quarter = chans // n
    half = quarter // 2
    steps = 2 * TAPS
    local = rows * width
    pair = 2 * width
    d = lax.axis_index("dp")
    h = lax.axis_index("height")
    core = lax.rem(d, 2)
    xor1 = h + 1 - 2 * lax.rem(h, 2)
    xor2 = lax.rem(h + 2, n)
    xor3 = xor1 + 2 - 4 * (xor1 // 2)
    other = d + 1 - 2 * core
    peers = (xor1, xor2, xor3)
    plane = lax.rem(d // 2, 2)
    across = d + 2 - 4 * plane

    def start_remote(src, dst, send, recv, dd, hh):
        return pltpu.make_async_remote_copy(
            src_ref=src, dst_ref=dst, send_sem=send, recv_sem=recv,
            device_id={"dp": dd, "height": hh},
            device_id_type=pl.DeviceIdType.MESH,
        )

    barrier = pltpu.get_barrier_semaphore()
    for hh in peers:
        pl.semaphore_signal(barrier, inc=1, device_id={"dp": d, "height": hh}, device_id_type=pl.DeviceIdType.MESH)
    pl.semaphore_signal(barrier, inc=1, device_id={"dp": other, "height": h}, device_id_type=pl.DeviceIdType.MESH)

    pl.semaphore_signal(barrier, inc=1, device_id={"dp": across, "height": h}, device_id_type=pl.DeviceIdType.MESH)

    loads = [
        pltpu.make_async_copy(lat.at[0], field.at[0, pl.ds(1, rows)], load_sem.at[0]),
        pltpu.make_async_copy(tan.at[0], field.at[1, pl.ds(1, rows)], load_sem.at[1]),
    ] + [
        pltpu.make_async_copy(
            w.at[pl.ds(3 * src, 3)],
            full.at[pl.ds(TAPS * i + 3 * dst, 3), pl.ds(pl.multiple_of(h * quarter, 16), quarter)],
            load_sem.at[2 + 3 * i + dst])
        for i, w in enumerate((weight_a, weight_b)) for dst, src in enumerate((1, 0, 2))
    ]
    for c in loads:
        c.start()
    def rows_of(hh, cc):
        return pl.ds(pl.multiple_of(hh * quarter + cc * half, 16), half)

    def shared(s):
        return SHARED[s] == 1

    def fetched(s, side):
        return not shared(s) or SIDE[s] == side

    corner = jnp.logical_or(h == 0, h == n - 1)
    turn_source = jnp.where(corner, xor2, xor1)
    turn_target = jnp.where(corner, xor1, xor2)

    def tap_of(v):
        part = lax.rem(v, TAPS)
        row = part // 3
        return 1 - row + 3 * (row // 2), lax.rem(part, 3)

    def own_copy(s, k, w=None, tap=None):
        if w is None:
            src = full.at[s, rows_of(h, core)]
        else:
            src = w.at[tap, pl.ds(pl.multiple_of(core * half, 16), half)]
        return start_remote(
            src, full.at[s, rows_of(h, core)],
            own_send.at[s, k], near_recv.at[s, k], d, peers[k])

    def relay_copy(s):
        turn = TURN[s] == 1
        block = full.at[s, rows_of(turn_source if turn else xor1, core)]
        return start_remote(block, block, relay_send.at[s], far_recv.at[s], d, turn_target if turn else xor2)

    def pair_copy(s, k):
        block = full.at[s, rows_of(peers[k], core)]
        return start_remote(block, block, pair_send.at[s, k], pair_recv.at[s, k], other, h)

    def plane_copy(s, k):
        block = full.at[s, rows_of(peers[k], core)]
        return start_remote(block, block, plane_send.at[s, k], plane_recv.at[s, k], across, h)

    def send_own(s, side):
        if fetched(s, side):
            p, q = (1, 0, 2)[s % TAPS // 3], s % 3
            for k in range(2):
                own_copy(s, k, (weight_a, weight_b)[s // TAPS], 3 * p + q).start()

    def pass_on(s, k):
        pair_copy(s, k).start()
        if shared(s):
            plane_copy(s, k).start()

    def relay(s, side):
        if fetched(s, side):
            for k in range(2):
                own_copy(s, k).wait_recv()
            relay_copy(s).start()
            for k in range(2):
                pass_on(s, k)

    def spread(s, side):
        if fetched(s, side):
            relay_copy(s).wait_recv()
            pass_on(s, 2)

    def mirror(s, side):
        if not fetched(s, side):
            for k in range(3):
                plane_copy(s, k).wait_recv()
                pair_copy(s, k).start()

    def both_planes(work):
        for side in range(2):
            @pl.when(plane == side)
            def _(side=side):
                for action, s in work:
                    action(s, side)

    def tick(t):
        work = []
        for action, table in ((mirror, CROSS), (spread, LATE), (relay, NEAR), (send_own, OWN)):
            before = table[t - 1] if t else FIRST if table is OWN else 0
            work += [(action, s) for s in range(before, table[t])]
        if work:
            both_planes(work)

    def loop(low, high, body):
        def one(v, carry):
            body(v)
            return carry
        lax.fori_loop(low, high, one, 0)

    def ticks(v, low, high, offset):
        for u in range(low, high):
            @pl.when(v == u)
            def _(u=u):
                tick(u + offset)

    def halo_copies(buf, k):
        top = [start_remote(buf.at[f, 1], buf.at[f, rows + 1], halo_send.at[k, 0, f], halo_recv.at[k, 0, f], d, lax.rem(h + n - 1, n)) for f in range(2)]
        low = [start_remote(buf.at[f, rows], buf.at[f, 0], halo_send.at[k, 1, f], halo_recv.at[k, 1, f], d, lax.rem(h + 1, n)) for f in range(2)]
        return top, low

    def halo_start(buf, k, sources=None, fields=(0, 1)):
        def edge_row(f, r):
            return buf.at[f, 1 + r] if sources is None else sources[f].at[0, r]

        @pl.when(h > 0)
        def _():
            for f in fields:
                start_remote(edge_row(f, 0), buf.at[f, rows + 1], halo_send.at[k, 0, f], halo_recv.at[k, 0, f], d, lax.rem(h + n - 1, n)).start()

        @pl.when(h < n - 1)
        def _():
            for f in fields:
                start_remote(edge_row(f, rows - 1), buf.at[f, 0], halo_send.at[k, 1, f], halo_recv.at[k, 1, f], d, lax.rem(h + 1, n)).start()

    def halo_wait(buf, k):
        top, low = halo_copies(buf, k)

        @pl.when(h > 0)
        def _():
            for c in top:
                c.wait_send()
            for c in low:
                c.wait_recv()

        @pl.when(h < n - 1)
        def _():
            for c in low:
                c.wait_send()
            for c in top:
                c.wait_recv()

    def local_stats(buf, k):
        zero = jnp.zeros((1, chans), F32)

        def sums(r, carry):
            return (
                carry[0] + jnp.sum(buf[0, r].astype(F32), axis=0, keepdims=True),
                carry[1] + jnp.sum(buf[1, r].astype(F32), axis=0, keepdims=True),
            )

        total, dtotal = lax.fori_loop(1, rows + 1, sums, (zero, zero))
        mean = total / local
        dmean = dtotal / local

        def moments(r, carry):
            v = buf[0, r].astype(F32) - mean
            dv = buf[1, r].astype(F32) - dmean
            return (
                carry[0] + jnp.sum(v * v, axis=0, keepdims=True),
                carry[1] + jnp.sum(v * dv, axis=0, keepdims=True),
            )

        second, dsecond = lax.fori_loop(1, rows + 1, moments, (zero, zero))
        stat[k, 0:1] = mean
        stat[k, 1:2] = dmean
        stat[k, 2:3] = second
        stat[k, 3:4] = dsecond
        stat[k, 4:8] = jnp.zeros((4, chans), F32)

    def stat_copy(k, j):
        return start_remote(stat.at[k], peer_stat.at[k, j], stat_send.at[k, j], stat_recv.at[k, j], d, peers[j])

    def group_sum(x):
        high = x.astype(BF16)
        rest = x - high.astype(F32)
        middle = rest.astype(BF16)
        low = (rest - middle.astype(F32)).astype(BF16)
        dot = lambda part: jnp.dot(part, same_group[...], preferred_element_type=F32)
        return dot(high) + dot(middle) + dot(low)

    def coefficients(k, gain):
        gain_row = gain[...].reshape(1, chans)
        for j in range(n - 1):
            stat_copy(k, j).wait_recv()
        size = chans // GROUPS
        blocks = [stat[k]] + [peer_stat[k, j] for j in range(n - 1)]
        both = blocks[0]
        for b in blocks[1:]:
            both = both + b
        means = group_sum(both) / (n * size)
        mean, dmean = means[0:1], means[1:2]
        var = jnp.zeros((1, chans), F32)
        dvar = jnp.zeros((1, chans), F32)
        for b in blocks:
            off = b[0:1] - mean
            doff = b[1:2] - dmean
            var = var + (b[2:3] + local * (off * off))
            dvar = dvar + (b[3:4] + local * (off * doff))
        row = lax.broadcasted_iota(jnp.int32, (8, chans), 0)
        packed = jnp.where(row == 0, var, jnp.where(row == 1, dvar, 0.0))
        moments = group_sum(packed) / (n * size * local)
        inverse = lax.rsqrt(moments[0:1] + epsilon)
        scale = gain_row * inverse
        slope = gain_row * (moments[1:2] * inverse * inverse * inverse)
        return mean, dmean, scale, slope

    column = lax.broadcasted_iota(jnp.int32, (width, 1), 0)

    def activate(buf, r, coef, keep):
        mean, dmean, scale, slope = coef
        v = buf[0, r].astype(F32) - mean
        dv = buf[1, r].astype(F32) - dmean
        a = v * scale
        da = dv * scale - v * slope
        s = jax.nn.sigmoid(a)
        hid = a * s
        dhid = da * (s * (1.0 + a * (1.0 - s)))
        if keep is not None:
            hid = jnp.where(keep, hid, 0.0)
            dhid = jnp.where(keep, dhid, 0.0)
        for f, x in ((0, hid), (1, dhid)):
            at = pl.ds(pl.multiple_of(r * pair + f * width, 128), width)
            shifted[1, at] = x.astype(BF16)
            shifted[0, at] = jnp.where(column == 0, 0.0, pltpu.roll(x, 1, 0)).astype(BF16)
            shifted[2, at] = jnp.where(column == width - 1, 0.0, pltpu.roll(x, width - 1, 0)).astype(BF16)

    def activate_rows(buf, coef):
        def one(r, carry):
            activate(buf, r, coef, None)
            return carry
        lax.fori_loop(1, rows + 1, one, 0)

    def activate_halo(buf, coef):
        def one(e, carry):
            r = e * (rows + 1)
            edge = jnp.where(e == 0, 0, n - 1)
            activate(buf, r, coef, h != edge)
            return carry
        lax.fori_loop(0, 2, one, 0)

    def arrive(v):
        for k in range(3):
            pair_copy(v, k).wait_recv()

    def accumulate(v, src, dst, count):
        q = tap_of(v)[1]
        at = pl.ds(pl.multiple_of(dst * pair, 128), count * pair)
        acc[at] += lax.dot_general(
            shifted[q, pl.ds(pl.multiple_of(src * pair, 128), count * pair)], full[v],
            (((1,), (1,)), ((), ())), preferred_element_type=F32)

    def center(low, high, offset):
        def one(v):
            ticks(v, low, high, offset)
            arrive(v)
            accumulate(v, 1, 0, rows)
        loop(low, high, one)

    def inner(low, high, offset):
        def one(v):
            ticks(v, low, high, offset)
            arrive(v)
            p = tap_of(v)[0]
            accumulate(v, 1 + p // 2, 1 - p // 2, rows - 1)
        loop(low, high, one)

    def edge(*taps):
        low = tap_of(taps[0])[0] // 2
        src = pl.ds(pl.multiple_of(low * (rows + 1) * pair, 128), pair)
        at = pl.ds(pl.multiple_of(low * (rows - 1) * pair, 128), pair)
        acc[at] += lax.dot_general(
            jnp.concatenate([shifted[tap_of(v)[1], src] for v in taps], axis=1),
            jnp.concatenate([full[v] for v in taps], axis=1),
            (((1,), (1,)), ((), ())), preferred_element_type=F32)

    loads[0].wait()
    loads[1].wait()
    local_stats(field, 0)
    pl.semaphore_wait(barrier, n + 1)
    for j in range(n - 1):
        stat_copy(0, j).start()
    both_planes([(send_own, s) for s in range(FIRST)])
    tick(0)
    acc[...] = jnp.zeros_like(acc)
    coef = coefficients(0, gain_a)
    tick(1)
    halo_start(field, 0, (lat, tan), (0,))
    activate_rows(field, coef)
    for c in loads[2:5]:
        c.wait()
    center(0, 1, 2)
    halo_start(field, 0, (lat, tan), (1,))
    center(1, 3, 2)
    inner(3, 9, 2)
    tick(11)
    halo_wait(field, 0)
    activate_halo(field, coef)
    edge(3, 4, 5)
    edge(6, 7, 8)

    for c in loads[5:]:
        c.wait()
    for f in range(2):
        for r in range(rows):
            at = r * pair + f * width
            mid[f, r + 1] = acc[at:at + width].astype(BF16)
    local_stats(mid, 1)
    for j in range(n - 1):
        stat_copy(1, j).start()
    tick(12)
    halo_start(mid, 1, None, (0,))
    acc[...] = jnp.zeros_like(acc)
    coef = coefficients(1, gain_b)
    tick(13)
    halo_start(mid, 1, None, (1,))
    activate_rows(mid, coef)
    center(TAPS, TAPS + 3, 5)
    inner(TAPS + 3, 17, 5)
    halo_wait(mid, 1)
    activate_halo(mid, coef)
    edge(12, 13, 14)
    edge(15, 16)
    tick(22)
    arrive(steps - 1)
    accumulate(steps - 1, 2, 0, rows)

    for f, o in ((0, out), (1, dout)):
        for r in range(rows):
            at = r * pair + f * width
            o[0, r] = (field[f, r + 1].astype(F32) + acc[at:at + width]).astype(BF16)

    def drain(s, side):
        if fetched(s, side):
            for k in range(2):
                own_copy(s, k).wait_send()
            relay_copy(s).wait_send()
            if shared(s):
                for k in range(3):
                    plane_copy(s, k).wait_send()
        for k in range(3):
            pair_copy(s, k).wait_send()
    both_planes([(drain, s) for s in range(steps)])
    for k in range(2):
        for j in range(n - 1):
            stat_copy(k, j).wait_send()


def fused(n, latents, latent_tangent, gain_first, weight_first, gain_second, weight_second):
    rows, width, chans = latents.shape[1:]
    size = chans // GROUPS
    group = np.arange(chans) // size
    same_group = jnp.asarray(group[:, None] == group[None, :], BF16)
    vmem = pl.BlockSpec(memory_space=pltpu.VMEM)
    hbm = pl.BlockSpec(memory_space=pl.ANY)
    dma = pltpu.SemaphoreType.DMA
    steps = 2 * TAPS
    shape = jax.ShapeDtypeStruct(latents.shape, BF16)
    return pl.pallas_call(
        functools.partial(fused_kernel, n),
        out_shape=(pltpu.VMEM(latents.shape, BF16), pltpu.VMEM(latents.shape, BF16)),
        in_specs=[hbm, hbm, vmem, vmem, hbm, hbm, vmem],
        out_specs=(vmem, vmem),
        scratch_shapes=[
            pltpu.VMEM((2, rows + 2, width, chans), BF16),
            pltpu.VMEM((2, rows + 2, width, chans), BF16),
            pltpu.VMEM((3, (rows + 2) * 2 * width, chans), BF16),
            pltpu.VMEM((2 * rows * width, chans), F32),
            pltpu.VMEM((steps, chans, chans), BF16),
            pltpu.VMEM((2, 8, chans), F32),
            pltpu.VMEM((2, n - 1, 8, chans), F32),
            dma((8,)),
            dma((2, 2, 2)),
            dma((2, 2, 2)),
            dma((2, n - 1)),
            dma((2, n - 1)),
            dma((steps, 2)),
            dma((steps, 2)),
            dma((steps,)),
            dma((steps,)),
            dma((steps, 3)),
            dma((steps, 3)),
            dma((steps, 3)),
            dma((steps, 3)),
        ],
        compiler_params=pltpu.CompilerParams(
            collective_id=0, has_side_effects=True, vmem_limit_bytes=61 * 1024 * 1024),
    )(
        latents, latent_tangent, gain_first, gain_second,
        weight_first.transpose(0, 2, 1), weight_second.transpose(0, 2, 1), same_group)


def extended(cells, sides, width):
    for axis, dim in sides:
        count = lax.axis_size(axis)
        ends = count - 1
        head = lax.slice_in_dim(cells, 0, width, axis=dim)
        tail = lax.slice_in_dim(cells, cells.shape[dim] - width, cells.shape[dim], axis=dim)
        cells = jnp.concatenate(
            [
                lax.ppermute(tail, axis, [(i, (i + 1) % count) for i in range(ends)]),
                cells,
                lax.ppermute(head, axis, [((i + 1) % count, i) for i in range(ends)]),
            ],
            axis=dim,
        )
    return cells


def normalize(stacked, gain_vector):
    row_count, col_count, chans = (stacked.shape[1], stacked.shape[2], stacked.shape[3])
    size = chans // GROUPS
    positions = float(row_count * col_count * size * lax.axis_size("height"))
    grouped = stacked.reshape(2, row_count * col_count, GROUPS, size)
    primal = grouped[0]
    tangent = grouped[1]
    first_totals = lax.psum((jnp.sum(primal, axis=(0, 2)), jnp.sum(tangent, axis=(0, 2))), "height")
    group_mean = first_totals[0] / positions
    tangent_mean = first_totals[1] / positions
    centered = primal - group_mean[None, :, None]
    tangent_centered = tangent - tangent_mean[None, :, None]
    second_totals = lax.psum(
        (
            jnp.sum(centered * centered, axis=(0, 2)),
            jnp.sum(centered * tangent_centered, axis=(0, 2)),
        ),
        "height",
    )
    variance = second_totals[0] / positions
    dvariance = 2.0 * second_totals[1] / positions
    inverse = lax.rsqrt(variance + epsilon)[None, :, None]
    normed = centered * inverse
    dnormed = tangent_centered * inverse - centered * (0.5 * dvariance[None, :, None] * inverse**3)
    scaled = normed.reshape(row_count, col_count, chans) * gain_vector
    dscaled = dnormed.reshape(row_count, col_count, chans) * gain_vector
    sigmoid_value = jax.nn.sigmoid(scaled)
    hidden = scaled * sigmoid_value
    dhidden = dscaled * sigmoid_value * (1.0 + scaled * (1.0 - sigmoid_value))
    return jnp.stack([hidden, dhidden], 0).astype(jnp.bfloat16)


def apply_taps(padded, weight_piece, row_count, col_count):
    chans = padded.shape[3]
    accumulated = jnp.zeros((2 * row_count * col_count, weight_piece.shape[2]), jnp.float32)
    for tap_index in range(9):
        offset_row = tap_index // 3
        offset_col = tap_index % 3
        window = padded[
            :, offset_row : offset_row + row_count, offset_col : offset_col + col_count, :
        ].reshape(-1, chans)
        accumulated = accumulated + jnp.dot(
            window, weight_piece[tap_index], preferred_element_type=jnp.float32
        )
    return accumulated


def convolve(hidden, weight):
    row_count, col_count = (hidden.shape[1], hidden.shape[2])
    padded = extended(hidden, (("height", 1),), 1)
    padded = jnp.pad(padded, ((0, 0), (0, 0), (1, 1), (0, 0)))
    flattened = apply_taps(
        padded, lax.all_gather(weight, "height", axis=2, tiled=True), row_count, col_count
    )
    return flattened.reshape(2, row_count, col_count, -1)


def per_device(latents, latent_tangent, gain_first, weight_first, gain_second, weight_second):
    stacked = jnp.concatenate([latents, latent_tangent], 0).astype(jnp.float32)
    hidden = normalize(stacked, gain_first)
    middle = convolve(hidden, weight_first).astype(jnp.bfloat16)
    second = normalize(middle.astype(jnp.float32), gain_second)
    result = (stacked + convolve(second, weight_second)).astype(jnp.bfloat16)
    return (result[0:1], result[1:2])


def solution(mesh):
    placed = (
        P("dp", "height", None, None),
        P("dp", "height", None, None),
        P(),
        P(None, None, "height"),
        P(),
        P(None, None, "height"),
    )
    n = mesh.shape["height"]
    body = per_device
    if n == 4 and mesh.shape["dp"] % 4 == 0:
        body = functools.partial(fused, n)
    return jax.shard_map(
        body,
        mesh=mesh,
        in_specs=placed,
        out_specs=(P("dp", "height", None, None), P("dp", "height", None, None)),
        check_vma=False,
    )
```
